8 devices in a mesh: fsdp: 4 (over z, y, x), tp: 2 (over core).
Axes of the slice: x: 2, y: 2, z: 1, core: 2. Of those that a mesh axis runs over, the one named last changes fastest.
Arguments:
- x: bfloat16 [32768, 5120], P(('fsdp', 'tp'))
- gamma: float32 [5120], replicated
- w1: bfloat16 [5120, 13824], P('fsdp', 'tp')
- w2: bfloat16 [13824, 5120], P('tp', 'fsdp')
Outputs:
- output: bfloat16 [32768, 5120], P(('fsdp', 'tp'))
All inputs are finite; a program needn't handle non-finite values.
Results may differ from the reference program's by a relative error of at most 0.001.
Values are sent between devices in bfloat16 or wider.
A program may use at most 1 GiB of HBM per device.

```python
import jax
import jax.numpy as jnp
from jax import lax

D = 5120
F = 13824
ROWS = 4096
FSDP = 4
TP = 2

TOK = FSDP * TP * ROWS
BLK = min(ROWS, 512)
EPS = 1e-6


def setup_inputs(seed: int = 0) -> dict:
    k = jax.random.split(jax.random.key(seed), 4)
    x = jax.random.normal(k[0], (TOK, D), jnp.float32).astype(jnp.bfloat16)
    gamma = jax.random.uniform(k[1], (D,), jnp.float32, 0.5, 1.5)
    w1 = (jax.random.normal(k[2], (D, F), jnp.float32) * D ** -0.5).astype(jnp.bfloat16)
    w2 = (jax.random.normal(k[3], (F, D), jnp.float32) * F ** -0.5).astype(jnp.bfloat16)
    return {"x": x, "gamma": gamma, "w1": w1, "w2": w2}


def _block(x, gamma, w1, w2):
    xf = x.astype(jnp.float32)
    mu = jnp.mean(xf, axis=-1, keepdims=True)
    var = jnp.mean(jnp.square(xf - mu), axis=-1, keepdims=True)
    xn = ((xf - mu) * lax.rsqrt(var + EPS) * gamma).astype(jnp.bfloat16)
    h = jax.nn.gelu(jnp.dot(xn, w1, preferred_element_type=jnp.float32), approximate=True).astype(jnp.bfloat16)
    y = jnp.dot(h, w2, preferred_element_type=jnp.float32)
    return (xf + y).astype(jnp.bfloat16)


def reference(x, gamma, w1, w2):
    xb = x.reshape(TOK // BLK, BLK, D)
    yb = lax.map(lambda blk: _block(blk, gamma, w1, w2), xb)
    return yb.reshape(TOK, D)
```

```python
import jax
import jax.numpy as jnp
from jax import lax
from jax.experimental import pallas as pl
from jax.experimental.pallas import tpu as pltpu
from jax.sharding import PartitionSpec as P

EPS = 1e-6
MESH = pl.DeviceIdType.MESH
BF16 = jnp.bfloat16
F32 = jnp.float32

ROWS, D, F = 4096, 5120, 13824
DS, FS = D // 4, F // 2
CH = 256
NCH = FS // CH
LB, LS = 256, 32
MB = 1024
NM = ROWS // MB
HB = 256
NH = ROWS // HB
MD, ND = 512, 256
GS = 64
TC = 256
NT = DS // TC
GT = 3
NG = -(-4 * NT // GT)
FH = FS // 2


def _mo(v, m):
    return pl.multiple_of(v, m)


def _kernel(x_ref, g_ref, w1_ref, w2_ref, y_ref, w1g, w2g, h_ref, ss, r1, r2, lx, lw, lh, l2w, l2x, l2y):
    a = lax.axis_index("fsdp")
    b = lax.axis_index("tp")
    ay, ax = a // 2, a % 2
    ob = 1 - b

    def nb(ry, rx):
        return ((ay + ry) % 2) * 2 + (ax + rx) % 2

    aX, aY, aD = nb(0, 1), nb(1, 0), nb(1, 1)
    devX, devY, devS = (aX, b), (aY, b), (a, ob)

    bar = pltpu.get_barrier_semaphore()
    for dev in (devX, devY, devS):
        pl.semaphore_signal(bar, inc=1, device_id=dev, device_id_type=MESH)
    pl.semaphore_wait(bar, 3)

    def send(src, dst, s, r, dev):
        pltpu.make_async_remote_copy(
            src_ref=src, dst_ref=dst, send_sem=s, recv_sem=r, device_id=dev, device_id_type=MESH
        ).start()

    def recv(dst, s, r, dev):
        pltpu.make_async_remote_copy(
            src_ref=dst, dst_ref=dst, send_sem=s, recv_sem=r, device_id=dev, device_id_type=MESH
        ).wait_recv()

    def w1_own(c):
        return w1_ref.at[:, pl.ds(_mo(c * CH, CH), CH)]

    def direct(c):
        send(w1_own(c), w1g.at[b, a, c], ss.at[0], r1.at[0, c], devX)
        send(w1_own(c), w1g.at[b, a, c], ss.at[1], r1.at[1, c], devY)
        send(w1_own(c), w1g.at[b, a, c], ss.at[4], r1.at[4, c], devS)

    def on_direct(c):
        recv(w1g.at[b, aX, c], ss.at[0], r1.at[0, c], devX)
        recv(w1g.at[b, aY, c], ss.at[1], r1.at[1, c], devY)
        top, bot = pl.ds(0, DS // 2), pl.ds(DS // 2, DS // 2)
        send(w1g.at[b, aY, c, top], w1g.at[b, aY, c, top], ss.at[2], r1.at[2, c], devX)
        send(w1g.at[b, aX, c, bot], w1g.at[b, aX, c, bot], ss.at[3], r1.at[3, c], devY)
        send(w1g.at[b, aX, c], w1g.at[b, aX, c], ss.at[5], r1.at[5, c], devS)
        send(w1g.at[b, aY, c], w1g.at[b, aY, c], ss.at[6], r1.at[6, c], devS)

    def on_relay(c):
        top, bot = pl.ds(0, DS // 2), pl.ds(DS // 2, DS // 2)
        recv(w1g.at[b, aD, c, top], ss.at[2], r1.at[2, c], devX)
        recv(w1g.at[b, aD, c, bot], ss.at[3], r1.at[3, c], devY)
        send(w1g.at[b, aD, c], w1g.at[b, aD, c], ss.at[7], r1.at[7, c], devS)

    def on_sib(c):
        for k, s in ((4, a), (5, aX), (6, aY), (7, aD)):
            recv(w1g.at[ob, s, c], ss.at[k], r1.at[k, c], devS)

    def cols(t):
        return pl.ds(_mo(t * TC, TC), TC)

    def w2_at(bb, s, t, rows=None):
        return w2g.at[bb, s, slice(None) if rows is None else rows, cols(t)]

    def w2_direct(t):
        send(w2_ref.at[:, cols(t)], w2_at(b, a, t), ss.at[8], r2.at[0, t], devX)
        send(w2_ref.at[:, cols(t)], w2_at(b, a, t), ss.at[9], r2.at[1, t], devY)

    def w2_sib_own(t):
        send(w2_ref.at[:, cols(t)], w2_at(b, a, t), ss.at[12], r2.at[4, t], devS)

    def w2_got_direct(t):
        for k, s, dev in ((0, aX, devX), (1, aY, devY)):
            recv(w2_at(b, s, t), ss.at[8 + k], r2.at[k, t], dev)
            send(w2_at(b, s, t), w2_at(b, s, t), ss.at[13 + k], r2.at[5 + k, t], devS)

    def w2_relay(t):
        for k, s, dev in ((0, aY, devX), (1, aX, devY)):
            v = w2_at(b, s, t, pl.ds(k * FH, FH))
            send(v, v, ss.at[10 + k], r2.at[2 + k, t], dev)

    def w2_got_relay(t):
        for k, dev in ((0, devX), (1, devY)):
            recv(w2_at(b, aD, t, pl.ds(k * FH, FH)), ss.at[10 + k], r2.at[2 + k, t], dev)
        send(w2_at(b, aD, t), w2_at(b, aD, t), ss.at[15], r2.at[7, t], devS)

    def w2_got_sib(rel, t):
        recv(w2_at(ob, (a, aX, aY, aD)[rel], t), ss.at[12 + rel], r2.at[4 + rel, t], devS)

    def upto(f, lo, hi):
        lax.fori_loop(lo, hi, lambda c, _: (f(c), 0)[1], 0)

    def lead(j):
        return jnp.minimum(NCH - 1, j + 1 + j // 14)

    def phase1(xn, gm, wb, acc0, acc1, hb):
        def x_load(i):
            rows = pl.ds(_mo(i * LB, LB), LB)
            return pltpu.make_async_copy(x_ref.at[rows, :], xn.at[rows, :], lx.at[i])

        direct(0)
        gcp = pltpu.make_async_copy(g_ref, gm, lx.at[ROWS // LB])
        gcp.start()

        @pl.loop(0, ROWS // LB)
        def _(i):
            x_load(i).start()

        gcp.wait()

        @pl.loop(0, ROWS // LB)
        def _(i):
            x_load(i).wait()

            @pl.when(i == 7)
            def _():
                on_direct(0)
                direct(1)
                direct(2)

            @pl.loop(0, LB // LS)
            def _(t):
                rows = pl.ds(_mo(i * LB + t * LS, LS), LS)
                xf = xn[rows, :].astype(F32)
                mu = jnp.mean(xf, axis=-1, keepdims=True)
                xc = xf - mu
                var = jnp.mean(jnp.square(xc), axis=-1, keepdims=True)
                xn[rows, :] = (xc * lax.rsqrt(var + EPS) * gm[0:1, :]).astype(BF16)

        def w_load(c, s):
            own, sib = pl.ds(0, CH), pl.ds(CH, CH)

            def rows(v):
                return pl.ds(_mo(v * DS, DS), DS)

            def cp(src, dst):
                pltpu.make_async_copy(src, dst, lw.at[s]).start()

            cp(w1_own(c), wb.at[s, rows(a), own])
            for v in (aX, aY, aD):
                cp(w1g.at[b, v, c], wb.at[s, rows(v), own])
            for v in (a, aX, aY, aD):
                cp(w1g.at[ob, v, c], wb.at[s, rows(v), sib])

        def h_store(j, m, s, half):
            off = (b if half == 0 else ob) * FS + j * CH
            return pltpu.make_async_copy(
                hb.at[s, half],
                h_ref.at[pl.ds(_mo(m * MB, MB), MB), pl.ds(_mo(off, CH), CH)],
                lh.at[s, half],
            )

        on_relay(0)
        on_sib(0)
        w_load(0, 0)
        acc1[...] = jnp.zeros_like(acc1)

        accs = (acc0, acc1)

        def finish(u):
            for r in range(0, MB, GS):
                for half in (0, 1):
                    v = accs[u][r : r + GS, half * CH : (half + 1) * CH]
                    hb[u, half, r : r + GS] = jax.nn.gelu(v, approximate=True).astype(BF16)

        def store(t, u):
            for half in (0, 1):
                h_store(t // NM, t % NM, u, half).start()

        def stored(u):
            for half in (0, 1):
                h_store(0, 0, u, half).wait()

        def events(j, m, s):
            more = j + 1 < NCH
            if m == 0:

                def take(c):
                    on_direct(c)

                    @pl.when(c + 2 < NCH)
                    def _():
                        direct(c + 2)

                upto(take, jnp.where(j == 0, 1, lead(j - 1) + 1), lead(j) + 1)
            if m == 1:

                @pl.when((j >= 14) & (j < 14 + NT))
                def _():
                    w2_sib_own(j - 14)

                @pl.when(j == NCH - 3)
                def _():
                    w2_direct(0)
                    w2_direct(1)

            if m == 2:

                @pl.when(more)
                def _():
                    on_relay(j + 1)

            if m == 3:

                @pl.when(more)
                def _():
                    on_sib(j + 1)
                    w_load(j + 1, 1 - s)

        @pl.loop(0, NCH)
        def _(j):
            s = j % 2
            pltpu.make_async_copy(wb.at[1 - s], wb.at[s], lw.at[s]).wait()

            @pl.loop(0, NM // 2)
            def _(m2):
                for u in (0, 1):
                    t = j * NM + m2 * 2 + u

                    for em in (u, u + 2):

                        @pl.when(m2 == em // 2)
                        def _(em=em):
                            events(j, em, s)

                    @pl.when(t > 2)
                    def _(u=u):
                        stored(1 - u)

                    finish(1 - u)
                    for r in range(0, MB, MD):
                        rows = pl.ds(_mo((m2 * 2 + u) * MB + r, MD), MD)
                        for c in range(0, 2 * CH, ND):
                            accs[u][r : r + MD, c : c + ND] = jnp.dot(
                                xn[rows, :], wb[s, :, c : c + ND], preferred_element_type=F32
                            )

                    @pl.when(t > 0)
                    def _(t=t, u=u):
                        store(t - 1, 1 - u)

        stored(1)
        finish(1)
        store(NCH * NM - 1, 1)
        for u in (0, 1):
            stored(u)

    pl.run_scoped(
        phase1,
        pltpu.VMEM((ROWS, D), BF16),
        pltpu.VMEM((8, D), F32),
        pltpu.VMEM((2, D, 2 * CH), BF16),
        pltpu.VMEM((MB, 2 * CH), F32),
        pltpu.VMEM((MB, 2 * CH), F32),
        pltpu.VMEM((2, 2, MB, CH), BF16),
    )

    def phase2(w0, w1, hb, xb, yb):
        sets = (w0, w1)

        def shard_of(n):
            mid = n - NT
            rx = jnp.where(n < NT, 0, jnp.where(n < 3 * NT, 1 - mid % 2, 1))
            ry = jnp.where(n < NT, 0, jnp.where(n < 3 * NT, mid % 2, 1))
            t = jnp.where(n < NT, n, jnp.where(n < 3 * NT, mid // 2, n - 3 * NT))
            return nb(ry, rx), t

        def w_load(n):
            g, k = n // GT, n % GT
            dst, sem = sets[g % 2], l2w.at[g % 2]
            tc = pl.ds(k * TC, TC)
            mid = n - NT
            if n < NT:
                src, t, rel = w2_ref.at[:, cols(n)], n, 0
            elif n < 3 * NT:
                t, rel = mid // 2, 1 + mid % 2
                src = w2_at(b, (aX, aY)[mid % 2], t)
            else:
                t, rel = n - 3 * NT, 3
                src = w2_at(b, aD, t)
            w2_got_sib(rel, t)
            pltpu.make_async_copy(src, dst.at[pl.ds(_mo(b * FS, FS), FS), tc], sem).start()
            osrc = w2_at(ob, (a, aX, aY, aD)[rel], t)
            pltpu.make_async_copy(osrc, dst.at[pl.ds(_mo(ob * FS, FS), FS), tc], sem).start()

        def w_wait(p, nt):
            v = sets[p].at[:, pl.ds(0, nt * TC)]
            pltpu.make_async_copy(v, v, l2w.at[p]).wait()

        def h_load(i, s):
            return pltpu.make_async_copy(h_ref.at[pl.ds(_mo(i * HB, HB), HB), :], hb.at[s], lx.at[s])

        def tiles(g, i, s, x, nt):
            for k in range(nt):
                owner, t = shard_of(g * GT + k)
                there = pl.ds(_mo(i * HB, HB), HB), pl.ds(_mo(owner * DS + t * TC, TC), TC)
                here = s, slice(None), pl.ds(k * TC, TC)
                if x:
                    yield pltpu.make_async_copy(x_ref.at[there], xb.at[here], l2x.at[s, k])
                else:
                    yield pltpu.make_async_copy(yb.at[here], y_ref.at[there], l2y.at[s, k])

        def each(g, i, s, x, act, last=False):
            for k, c in enumerate(tiles(g, i, s, x, GT - last)):
                getattr(c, act)()

        ev = {
            (0, 0): lambda: (w2_direct(2), w_load(3), w_load(4)),
            (0, 4): lambda: w2_got_direct(0),
            (0, 6): lambda: w_load(5),
            (1, 0): lambda: (w2_got_direct(1), w2_direct(3), w_load(6)),
            (1, 3): lambda: (w_load(7), w_load(8)),
            (2, 0): lambda: (w2_got_direct(2), w2_direct(4)),
            (2, 3): lambda: (w_load(9), w_load(10)),
            (2, 11): lambda: (w2_got_direct(3), w2_relay(0), w2_relay(1)),
            (2, 13): lambda: w_load(11),
            (3, 0): lambda: w_load(12),
            (3, 8): lambda: (w2_got_direct(4), w2_relay(2), w2_relay(3), w2_relay(4)),
            (3, 10): lambda: (w_load(13), w_load(14)),
            (4, 1): lambda: w2_got_relay(0),
            (4, 3): lambda: w_load(15),
            (4, 6): lambda: w2_got_relay(1),
            (4, 8): lambda: w_load(16),
            (4, 12): lambda: w2_got_relay(2),
            (4, 14): lambda: w_load(17),
            (5, 2): lambda: w2_got_relay(3),
            (5, 5): lambda: w_load(18),
            (5, 9): lambda: w2_got_relay(4),
            (5, 12): lambda: w_load(19),
        }

        h_load(0, 0).start()
        each(0, 0, 0, True, "start")
        for n in range(GT):
            w_load(n)

        def group(g, p, last):
            nt = 4 * NT - GT * (NG - 1) if last else GT
            w_wait(p, nt)

            @pl.loop(0, NH)
            def _(i):
                s = i % 2
                if not last:
                    h_load((i + 1) % NH, 1 - s).start()

                    @pl.when(i + 1 < NH)
                    def _():
                        each(g, i + 1, 1 - s, True, "start")

                    @pl.when((i + 1 == NH) & (g < NG - 2))
                    def _():
                        each(g + 1, 0, 0, True, "start")

                    @pl.when((i + 1 == NH) & (g == NG - 2))
                    def _():
                        each(NG - 1, 0, 0, True, "start", True)

                    for (eg, ei), f in ev.items():
                        if eg % 2 == p:

                            @pl.when((g == eg) & (i == ei))
                            def _(f=f):
                                f()
                else:

                    @pl.when(i + 1 < NH)
                    def _():
                        h_load(i + 1, 1 - s).start()
                        each(g, i + 1, 1 - s, True, "start", True)

                h_load(i, s).wait()
                each(g, i, s, True, "wait", last)
                if last:

                    @pl.when(i < 2)
                    def _():
                        each(NG - 2, i, s, False, "wait")

                    @pl.when(i > 1)
                    def _():
                        each(g, i, s, False, "wait", True)
                else:

                    @pl.when((g > 0) | (i > 1))
                    def _():
                        each(g, i, s, False, "wait")

                n = nt * TC
                d = jnp.dot(hb[s], sets[p][:, :n], preferred_element_type=F32)
                yb[s, :, :n] = (xb[s, :, :n].astype(F32) + d).astype(BF16)
                each(g, i, s, False, "start", last)

        @pl.loop(0, (NG - 1) // 2)
        def _(q):
            for p in (0, 1):
                group(2 * q + p, p, False)

        group(NG - 1, 0, True)
        for i in (0, 1):
            each(NG - 1, i, i, False, "wait", True)

    pl.run_scoped(
        phase2,
        pltpu.VMEM((F, GT * TC), BF16),
        pltpu.VMEM((F, GT * TC), BF16),
        pltpu.VMEM((2, HB, F), BF16),
        pltpu.VMEM((2, HB, GT * TC), BF16),
        pltpu.VMEM((2, HB, GT * TC), BF16),
    )

    def drain(ref, k):
        pltpu.make_async_copy(ref, ref, ss.at[k]).wait()

    for k in (0, 1, 4, 5, 6, 7):
        drain(w1_ref, k)
    for k in (2, 3):
        drain(w1_ref.at[pl.ds(0, DS // 2), :], k)
    for k in (8, 9, 12, 13, 14, 15):
        drain(w2_ref, k)
    for k in (10, 11):
        drain(w2_ref.at[pl.ds(0, FH), :], k)


def solution(mesh):
    any_spec = pl.BlockSpec(memory_space=pl.ANY)

    def body(x, gamma, w1, w2):
        y, _, _, _ = pl.pallas_call(
            _kernel,
            out_shape=(
                jax.ShapeDtypeStruct((ROWS, D), BF16),
                jax.ShapeDtypeStruct((2, 4, NCH, DS, CH), BF16),
                jax.ShapeDtypeStruct((2, 4, FS, DS), BF16),
                jax.ShapeDtypeStruct((ROWS, F), BF16),
            ),
            in_specs=[any_spec] * 4,
            out_specs=(any_spec,) * 4,
            scratch_shapes=[
                pltpu.SemaphoreType.DMA((16,)),
                pltpu.SemaphoreType.DMA((8, NCH)),
                pltpu.SemaphoreType.DMA((8, NT)),
                pltpu.SemaphoreType.DMA((ROWS // LB + 1,)),
                pltpu.SemaphoreType.DMA((2,)),
                pltpu.SemaphoreType.DMA((2, 2)),
                pltpu.SemaphoreType.DMA((2,)),
                pltpu.SemaphoreType.DMA((2, GT)),
                pltpu.SemaphoreType.DMA((2, GT)),
            ],
            compiler_params=pltpu.CompilerParams(
                collective_id=0, has_side_effects=True, vmem_limit_bytes=67043328
            ),
            cost_estimate=pl.CostEstimate(
                flops=4 * ROWS * D * F, bytes_accessed=2 * 10**9, transcendentals=ROWS * F
            ),
            name="mlp",
        )(x, jnp.broadcast_to(gamma, (8, D)), w1, w2)
        return y

    return jax.shard_map(
        body,
        mesh=mesh,
        in_specs=(P(("fsdp", "tp"), None), P(None), P("fsdp", "tp"), P("tp", "fsdp")),
        out_specs=P(("fsdp", "tp"), None),
        check_vma=False,
    )
```

```python
import jax
import jax.numpy as jnp
from jax import lax
from jax.experimental import pallas as pl
from jax.experimental.pallas import tpu as pltpu
from jax.sharding import PartitionSpec as P

EPS = 1e-6
MESH = pl.DeviceIdType.MESH
BF16 = jnp.bfloat16
F32 = jnp.float32

ROWS, D, F = 4096, 5120, 13824
DS, FS = D // 4, F // 2
CH = 256
NCH = FS // CH
LB, LS = 256, 32
MB = 1024
NM = ROWS // MB
HB = 256
NH = ROWS // HB
MD, ND = 512, 256
GS = 64
TC = 256
NT = DS // TC
GT = 3
NG = -(-4 * NT // GT)
FH = FS // 2


def _mo(v, m):
    return pl.multiple_of(v, m)


def _kernel(x_ref, g_ref, w1_ref, w2_ref, y_ref, w1g, w2g, h_ref, ss, r1, r2, lx, lw, lh, l2w, l2x, l2y):
    a = lax.axis_index("fsdp")
    b = lax.axis_index("tp")
    ay, ax = a // 2, a % 2
    ob = 1 - b

    def nb(ry, rx):
        return ((ay + ry) % 2) * 2 + (ax + rx) % 2

    aX, aY, aD = nb(0, 1), nb(1, 0), nb(1, 1)
    devX, devY, devS = (aX, b), (aY, b), (a, ob)

    bar = pltpu.get_barrier_semaphore()
    for dev in (devX, devY, devS):
        pl.semaphore_signal(bar, inc=1, device_id=dev, device_id_type=MESH)
    pl.semaphore_wait(bar, 3)

    def send(src, dst, s, r, dev):
        pltpu.make_async_remote_copy(
            src_ref=src, dst_ref=dst, send_sem=s, recv_sem=r, device_id=dev, device_id_type=MESH
        ).start()

    def recv(dst, s, r, dev):
        pltpu.make_async_remote_copy(
            src_ref=dst, dst_ref=dst, send_sem=s, recv_sem=r, device_id=dev, device_id_type=MESH
        ).wait_recv()

    def w1_own(c):
        return w1_ref.at[:, pl.ds(_mo(c * CH, CH), CH)]

    def direct(c):
        send(w1_own(c), w1g.at[b, a, c], ss.at[0], r1.at[0, c], devX)
        send(w1_own(c), w1g.at[b, a, c], ss.at[1], r1.at[1, c], devY)
        send(w1_own(c), w1g.at[b, a, c], ss.at[4], r1.at[4, c], devS)

    def on_direct(c):
        recv(w1g.at[b, aX, c], ss.at[0], r1.at[0, c], devX)
        recv(w1g.at[b, aY, c], ss.at[1], r1.at[1, c], devY)
        top, bot = pl.ds(0, DS // 2), pl.ds(DS // 2, DS // 2)
        send(w1g.at[b, aY, c, top], w1g.at[b, aY, c, top], ss.at[2], r1.at[2, c], devX)
        send(w1g.at[b, aX, c, bot], w1g.at[b, aX, c, bot], ss.at[3], r1.at[3, c], devY)
        send(w1g.at[b, aX, c], w1g.at[b, aX, c], ss.at[5], r1.at[5, c], devS)
        send(w1g.at[b, aY, c], w1g.at[b, aY, c], ss.at[6], r1.at[6, c], devS)

    def on_relay(c):
        top, bot = pl.ds(0, DS // 2), pl.ds(DS // 2, DS // 2)
        recv(w1g.at[b, aD, c, top], ss.at[2], r1.at[2, c], devX)
        recv(w1g.at[b, aD, c, bot], ss.at[3], r1.at[3, c], devY)
        send(w1g.at[b, aD, c], w1g.at[b, aD, c], ss.at[7], r1.at[7, c], devS)

    def on_sib(c):
        for k, s in ((4, a), (5, aX), (6, aY), (7, aD)):
            recv(w1g.at[ob, s, c], ss.at[k], r1.at[k, c], devS)

    def cols(t):
        return pl.ds(_mo(t * TC, TC), TC)

    def w2_at(bb, s, t, rows=None):
        return w2g.at[bb, s, slice(None) if rows is None else rows, cols(t)]

    def w2_direct(t):
        send(w2_ref.at[:, cols(t)], w2_at(b, a, t), ss.at[8], r2.at[0, t], devX)
        send(w2_ref.at[:, cols(t)], w2_at(b, a, t), ss.at[9], r2.at[1, t], devY)

    def w2_sib_own(t):
        send(w2_ref.at[:, cols(t)], w2_at(b, a, t), ss.at[12], r2.at[4, t], devS)

    def w2_got_direct(t):
        for k, s, dev in ((0, aX, devX), (1, aY, devY)):
            recv(w2_at(b, s, t), ss.at[8 + k], r2.at[k, t], dev)
            send(w2_at(b, s, t), w2_at(b, s, t), ss.at[13 + k], r2.at[5 + k, t], devS)

    def w2_relay(t):
        for k, s, dev in ((0, aY, devX), (1, aX, devY)):
            v = w2_at(b, s, t, pl.ds(k * FH, FH))
            send(v, v, ss.at[10 + k], r2.at[2 + k, t], dev)

    def w2_got_relay(t):
        for k, dev in ((0, devX), (1, devY)):
            recv(w2_at(b, aD, t, pl.ds(k * FH, FH)), ss.at[10 + k], r2.at[2 + k, t], dev)
        send(w2_at(b, aD, t), w2_at(b, aD, t), ss.at[15], r2.at[7, t], devS)

    def w2_got_sib(rel, t):
        recv(w2_at(ob, (a, aX, aY, aD)[rel], t), ss.at[12 + rel], r2.at[4 + rel, t], devS)

    def upto(f, lo, hi):
        lax.fori_loop(lo, hi, lambda c, _: (f(c), 0)[1], 0)

    def lead(j):
        return jnp.minimum(NCH - 1, j + 1 + j // 14)

    def phase1(xn, gm, wb, acc0, acc1, hb):
        def x_load(i):
            rows = pl.ds(_mo(i * LB, LB), LB)
            return pltpu.make_async_copy(x_ref.at[rows, :], xn.at[rows, :], lx.at[i])

        def w_load(c, s):
            own, sib = pl.ds(0, CH), pl.ds(CH, CH)

            def rows(v):
                return pl.ds(_mo(v * DS, DS), DS)

            def cp(src, dst):
                pltpu.make_async_copy(src, dst, lw.at[s]).start()

            cp(w1_own(c), wb.at[s, rows(a), own])
            for v in (aX, aY, aD):
                cp(w1g.at[b, v, c], wb.at[s, rows(v), own])
            for v in (a, aX, aY, aD):
                cp(w1g.at[ob, v, c], wb.at[s, rows(v), sib])

        direct(0)
        gcp = pltpu.make_async_copy(g_ref, gm, lx.at[ROWS // LB])
        gcp.start()

        @pl.loop(0, ROWS // LB)
        def _(i):
            x_load(i).start()

        gcp.wait()

        @pl.loop(0, ROWS // LB)
        def _(i):
            x_load(i).wait()

            @pl.when(i == 7)
            def _():
                on_direct(0)
                direct(1)
                direct(2)

            @pl.when(i == 12)
            def _():
                on_relay(0)

            @pl.when(i == 14)
            def _():
                on_sib(0)
                w_load(0, 0)

            @pl.loop(0, LB // LS)
            def _(t):
                rows = pl.ds(_mo(i * LB + t * LS, LS), LS)
                xf = xn[rows, :].astype(F32)
                mu = jnp.mean(xf, axis=-1, keepdims=True)
                xc = xf - mu
                var = jnp.mean(jnp.square(xc), axis=-1, keepdims=True)
                xn[rows, :] = (xc * lax.rsqrt(var + EPS) * gm[0:1, :]).astype(BF16)

        def h_store(j, m, s, half):
            off = (b if half == 0 else ob) * FS + j * CH
            return pltpu.make_async_copy(
                hb.at[s, half],
                h_ref.at[pl.ds(_mo(m * MB, MB), MB), pl.ds(_mo(off, CH), CH)],
                lh.at[s, half],
            )

        acc1[...] = jnp.zeros_like(acc1)

        accs = (acc0, acc1)

        def finish(u):
            for r in range(0, MB, GS):
                for half in (0, 1):
                    v = accs[u][r : r + GS, half * CH : (half + 1) * CH]
                    hb[u, half, r : r + GS] = jax.nn.gelu(v, approximate=True).astype(BF16)

        def store(t, u):
            for half in (0, 1):
                h_store(t // NM, t % NM, u, half).start()

        def stored(u):
            for half in (0, 1):
                h_store(0, 0, u, half).wait()

        def events(j, m, s):
            more = j + 1 < NCH
            if m == 0:

                def take(c):
                    on_direct(c)

                    @pl.when(c + 2 < NCH)
                    def _():
                        direct(c + 2)

                upto(take, jnp.where(j == 0, 1, lead(j - 1) + 1), lead(j) + 1)
            if m == 1:

                @pl.when((j >= 14) & (j < 14 + NT))
                def _():
                    w2_sib_own(j - 14)

                @pl.when(j == NCH - 3)
                def _():
                    w2_direct(0)
                    w2_direct(1)

            if m == 2:

                @pl.when(more)
                def _():
                    on_relay(j + 1)

            if m == 3:

                @pl.when(more)
                def _():
                    on_sib(j + 1)
                    w_load(j + 1, 1 - s)

        @pl.loop(0, NCH)
        def _(j):
            s = j % 2
            pltpu.make_async_copy(wb.at[1 - s], wb.at[s], lw.at[s]).wait()

            @pl.loop(0, NM // 2)
            def _(m2):
                for u in (0, 1):
                    t = j * NM + m2 * 2 + u

                    for em in (u, u + 2):

                        @pl.when(m2 == em // 2)
                        def _(em=em):
                            events(j, em, s)

                    @pl.when(t > 2)
                    def _(u=u):
                        stored(1 - u)

                    finish(1 - u)
                    for r in range(0, MB, MD):
                        rows = pl.ds(_mo((m2 * 2 + u) * MB + r, MD), MD)
                        for c in range(0, 2 * CH, ND):
                            accs[u][r : r + MD, c : c + ND] = jnp.dot(
                                xn[rows, :], wb[s, :, c : c + ND], preferred_element_type=F32
                            )

                    @pl.when(t > 0)
                    def _(t=t, u=u):
                        store(t - 1, 1 - u)

        stored(1)
        finish(1)
        store(NCH * NM - 1, 1)
        for u in (0, 1):
            stored(u)

    pl.run_scoped(
        phase1,
        pltpu.VMEM((ROWS, D), BF16),
        pltpu.VMEM((8, D), F32),
        pltpu.VMEM((2, D, 2 * CH), BF16),
        pltpu.VMEM((MB, 2 * CH), F32),
        pltpu.VMEM((MB, 2 * CH), F32),
        pltpu.VMEM((2, 2, MB, CH), BF16),
    )

    def phase2(w0, w1, hb, xb, yb):
        sets = (w0, w1)

        def shard_of(n):
            mid = n - NT
            rx = jnp.where(n < NT, 0, jnp.where(n < 3 * NT, 1 - mid % 2, 1))
            ry = jnp.where(n < NT, 0, jnp.where(n < 3 * NT, mid % 2, 1))
            t = jnp.where(n < NT, n, jnp.where(n < 3 * NT, mid // 2, n - 3 * NT))
            return nb(ry, rx), t

        def w_load(n):
            g, k = n // GT, n % GT
            dst, sem = sets[g % 2], l2w.at[g % 2]
            tc = pl.ds(k * TC, TC)
            mid = n - NT
            if n < NT:
                src, t, rel = w2_ref.at[:, cols(n)], n, 0
            elif n < 3 * NT:
                t, rel = mid // 2, 1 + mid % 2
                src = w2_at(b, (aX, aY)[mid % 2], t)
            else:
                t, rel = n - 3 * NT, 3
                src = w2_at(b, aD, t)
            w2_got_sib(rel, t)
            pltpu.make_async_copy(src, dst.at[pl.ds(_mo(b * FS, FS), FS), tc], sem).start()
            osrc = w2_at(ob, (a, aX, aY, aD)[rel], t)
            pltpu.make_async_copy(osrc, dst.at[pl.ds(_mo(ob * FS, FS), FS), tc], sem).start()

        def w_wait(p, nt):
            v = sets[p].at[:, pl.ds(0, nt * TC)]
            pltpu.make_async_copy(v, v, l2w.at[p]).wait()

        def h_load(i, s):
            return pltpu.make_async_copy(h_ref.at[pl.ds(_mo(i * HB, HB), HB), :], hb.at[s], lx.at[s])

        def tiles(g, i, s, x, nt):
            for k in range(nt):
                owner, t = shard_of(g * GT + k)
                there = pl.ds(_mo(i * HB, HB), HB), pl.ds(_mo(owner * DS + t * TC, TC), TC)
                here = s, slice(None), pl.ds(k * TC, TC)
                if x:
                    yield pltpu.make_async_copy(x_ref.at[there], xb.at[here], l2x.at[s, k])
                else:
                    yield pltpu.make_async_copy(yb.at[here], y_ref.at[there], l2y.at[s, k])

        def each(g, i, s, x, act, last=False):
            for c in tiles(g, i, s, x, GT - last):
                getattr(c, act)()

        ev = {
            (0, 0): lambda: (w2_direct(2), w_load(3), w_load(4)),
            (0, 4): lambda: w2_got_direct(0),
            (0, 6): lambda: w_load(5),
            (1, 0): lambda: (w2_got_direct(1), w2_direct(3), w_load(6)),
            (1, 3): lambda: (w_load(7), w_load(8)),
            (2, 0): lambda: (w2_got_direct(2), w2_direct(4)),
            (2, 3): lambda: (w_load(9), w_load(10)),
            (2, 11): lambda: (w2_got_direct(3), w2_relay(0), w2_relay(1)),
            (2, 13): lambda: w_load(11),
            (3, 0): lambda: w_load(12),
            (3, 8): lambda: (w2_got_direct(4), w2_relay(2), w2_relay(3), w2_relay(4)),
            (3, 10): lambda: (w_load(13), w_load(14)),
            (4, 1): lambda: w2_got_relay(0),
            (4, 3): lambda: w_load(15),
            (4, 6): lambda: w2_got_relay(1),
            (4, 8): lambda: w_load(16),
            (4, 12): lambda: w2_got_relay(2),
            (4, 14): lambda: w_load(17),
            (5, 2): lambda: w2_got_relay(3),
            (5, 5): lambda: w_load(18),
            (5, 9): lambda: w2_got_relay(4),
            (5, 12): lambda: w_load(19),
        }

        h_load(0, 0).start()
        each(0, 0, 0, True, "start")
        for n in range(GT):
            w_load(n)

        def group(g, p, last):
            nt = 4 * NT - GT * (NG - 1) if last else GT
            w_wait(p, nt)

            @pl.loop(0, NH)
            def _(i):
                s = i % 2
                if not last:
                    h_load((i + 1) % NH, 1 - s).start()

                    @pl.when(i + 1 < NH)
                    def _():
                        each(g, i + 1, 1 - s, True, "start")

                    @pl.when((i + 1 == NH) & (g < NG - 2))
                    def _():
                        each(g + 1, 0, 0, True, "start")

                    @pl.when((i + 1 == NH) & (g == NG - 2))
                    def _():
                        each(NG - 1, 0, 0, True, "start", True)

                    for eg in range(p, NG - 1, 2):

                        @pl.when(g == eg)
                        def _(eg=eg):
                            for (fg, ei), f in ev.items():
                                if fg == eg:
                                    @pl.when(i == ei)
                                    def _(f=f):
                                        f()
                else:

                    @pl.when(i + 1 < NH)
                    def _():
                        h_load(i + 1, 1 - s).start()
                        each(g, i + 1, 1 - s, True, "start", True)

                h_load(i, s).wait()
                each(g, i, s, True, "wait", last)
                if last:

                    @pl.when(i < 2)
                    def _():
                        each(NG - 2, i, s, False, "wait")

                    @pl.when(i > 1)
                    def _():
                        each(g, i, s, False, "wait", True)
                else:

                    @pl.when((g > 0) | (i > 1))
                    def _():
                        each(g, i, s, False, "wait")

                n = nt * TC
                d = jnp.dot(hb[s], sets[p][:, :n], preferred_element_type=F32)
                yb[s, :, :n] = (xb[s, :, :n].astype(F32) + d).astype(BF16)
                each(g, i, s, False, "start", last)

        @pl.loop(0, (NG - 1) // 2)
        def _(q):
            for p in (0, 1):
                group(2 * q + p, p, False)

        group(NG - 1, 0, True)
        for i in (0, 1):
            each(NG - 1, i, i, False, "wait", True)

    pl.run_scoped(
        phase2,
        pltpu.VMEM((F, GT * TC), BF16),
        pltpu.VMEM((F, GT * TC), BF16),
        pltpu.VMEM((2, HB, F), BF16),
        pltpu.VMEM((2, HB, GT * TC), BF16),
        pltpu.VMEM((2, HB, GT * TC), BF16),
    )

    def drain(ref, k):
        pltpu.make_async_copy(ref, ref, ss.at[k]).wait()

    for k in (0, 1, 4, 5, 6, 7):
        drain(w1_ref, k)
    for k in (2, 3):
        drain(w1_ref.at[pl.ds(0, DS // 2), :], k)
    for k in (8, 9, 12, 13, 14, 15):
        drain(w2_ref, k)
    for k in (10, 11):
        drain(w2_ref.at[pl.ds(0, FH), :], k)


def solution(mesh):
    any_spec = pl.BlockSpec(memory_space=pl.ANY)

    def body(x, gamma, w1, w2):
        y, _, _, _ = pl.pallas_call(
            _kernel,
            out_shape=(
                jax.ShapeDtypeStruct((ROWS, D), BF16),
                jax.ShapeDtypeStruct((2, 4, NCH, DS, CH), BF16),
                jax.ShapeDtypeStruct((2, 4, FS, DS), BF16),
                jax.ShapeDtypeStruct((ROWS, F), BF16),
            ),
            in_specs=[any_spec] * 4,
            out_specs=(any_spec,) * 4,
            scratch_shapes=[
                pltpu.SemaphoreType.DMA((16,)),
                pltpu.SemaphoreType.DMA((8, NCH)),
                pltpu.SemaphoreType.DMA((8, NT)),
                pltpu.SemaphoreType.DMA((ROWS // LB + 1,)),
                pltpu.SemaphoreType.DMA((2,)),
                pltpu.SemaphoreType.DMA((2, 2)),
                pltpu.SemaphoreType.DMA((2,)),
                pltpu.SemaphoreType.DMA((2, GT)),
                pltpu.SemaphoreType.DMA((2, GT)),
            ],
            compiler_params=pltpu.CompilerParams(
                collective_id=0, has_side_effects=True, vmem_limit_bytes=67043328
            ),
            cost_estimate=pl.CostEstimate(
                flops=4 * ROWS * D * F, bytes_accessed=2 * 10**9, transcendentals=ROWS * F
            ),
            name="mlp",
        )(x, jnp.broadcast_to(gamma, (8, D)), w1, w2)
        return y

    return jax.shard_map(
        body,
        mesh=mesh,
        in_specs=(P(("fsdp", "tp"), None), P(None), P("fsdp", "tp"), P("tp", "fsdp")),
        out_specs=P(("fsdp", "tp"), None),
        check_vma=False,
    )
```
